256 devices in a mesh: parts: 2 (over z), wide: 128 (over y, x, core).
Axes of the slice: x: 8, y: 8, z: 2, core: 2. Of those that a mesh axis runs over, the one named last changes fastest.
The devices are a block of a 8x8x16 slice.
Arguments:
- a_rows: bfloat16 [327680, 2048], P(('parts', 'wide')), parts along dimension 0, may hold values from -6 to 6
- xa_panel: bfloat16 [4096, 256], P(('parts', 'wide')), parts along dimension 0, may hold values from -0.125 to 0.125
- za_panel: bfloat16 [4096, 256], P(('parts', 'wide')), parts along dimension 0, may hold values from -0.125 to 0.125
- send_order: int32 [256, 1280], P(('parts', 'wide')), parts along dimension 0, may hold values from 0 to 1279, each once within a row
- recv_order: int32 [256, 1280], P(('parts', 'wide')), parts along dimension 0, may hold values from 0 to 1279, each once within a row
- shift: float32 [128], P('parts'), parts along dimension 0, may hold values from 1 to 8
- resident: bfloat16 [327680, 1024], P(('parts', 'wide')), parts along dimension 0, may hold values from -6 to 6
Outputs:
- factored: float32 [327680, 256], P(('parts', 'wide')), parts along dimension 0
- updated: bfloat16 [327680, 1024], P(('parts', 'wide')), parts along dimension 0
- pivots: float32 [128], P('parts'), parts along dimension 0
The draws below stay inside these ranges and needn't reach their ends.
There are 2 independent parts, one for each index of `parts`. The reference program is written for one: setup_inputs(seed, part) draws one part's arguments, and reference() takes and returns one part's arrays. A program takes and returns all parts, laid end to end along the dimension named above; each array names one. Nothing has to cross between parts.
Inputs may be any that keep to these rules, and one draw needn't show every extreme that they name: Each row of send_order is a permutation of the local constraint rows. Each row of recv_order is a permutation of the received slots.
All inputs are finite; a program needn't handle non-finite values.
Results may differ from the reference program's by a relative error of at most 0.0004.
Values may be sent and summed in bfloat16 or wider, within the bound.
A program may use at most 64 MiB of HBM per device.

```python
import math
import jax
import jax.numpy as jnp
from jax import lax

NV = 2048
COLS = 256
PANEL = 64
RES = 1024
R_DEV = 1280
M_ROWS = 163840
N_WIDE = 128


def block_scale(own_key, shape, cuts, low, largest):
    def one(dim, blocks):
        draws = jax.random.uniform(jax.random.fold_in(jax.random.fold_in(own_key, 6), dim), (blocks,), jnp.float32, low / len(cuts), largest / len(cuts))
        return jnp.repeat(jnp.exp(draws), shape[dim] // blocks).reshape((-1,) + (1,) * (len(shape) - dim - 1))

    loudness = one(*cuts[0])
    for cut in cuts[1:]:
        loudness = loudness * one(*cut)
    return loudness


def normal_values(rng, shape, scale, limit, pieces=(), kind=jnp.bfloat16):
    level = block_scale(rng, shape, pieces, -0.22, 0.18) if pieces else 1.0
    values = jax.random.normal(rng, shape, jnp.float32) * scale * level
    return jnp.minimum(jnp.maximum(values, -limit), limit).astype(kind)


def setup_inputs(seed: int = 0, part: int = 0) -> dict:
    key_list = jax.random.split(jax.random.key(seed), 8)
    own_keys = jax.random.split(jax.random.fold_in(key_list[7], part), 8)
    a_rows = normal_values(own_keys[0], (M_ROWS, NV), 1.0, 6.0, ((0, 128),))
    xa_panel = normal_values(own_keys[1], (NV, COLS), NV ** -0.5, 0.125, ((0, 128),))
    za_panel = normal_values(own_keys[2], (NV, COLS), NV ** -0.5, 0.125, ((0, 128),))
    send_order = jax.vmap(lambda own: jax.random.permutation(own, R_DEV))(jax.random.split(own_keys[3], N_WIDE)).reshape((N_WIDE, R_DEV)).astype(jnp.int32)
    recv_order = jax.vmap(lambda own: jax.random.permutation(own, R_DEV))(jax.random.split(own_keys[4], N_WIDE)).reshape((N_WIDE, R_DEV)).astype(jnp.int32)
    shift = jnp.clip(jnp.exp(jax.random.uniform(own_keys[5], (PANEL,), jnp.float32, math.log(1.0), math.log(8.0))), 1.0, 8.0)
    resident = normal_values(own_keys[6], (M_ROWS, RES), 1.0, 6.0, ((0, 128),))
    return dict(a_rows=a_rows, xa_panel=xa_panel, za_panel=za_panel, send_order=send_order, recv_order=recv_order, shift=shift, resident=resident)


def factor(block, shift):
    extent = block.shape[0]
    positions = jnp.arange(extent)
    mirrored = jnp.tril(block) + jnp.tril(block, -1).T
    magnitude = jnp.sum(jnp.abs(mirrored), axis=1)
    is_diag = positions[:, None] == positions[None, :]
    work = jnp.where(is_diag, (shift + magnitude)[:, None], mirrored)

    def step(column_index, carry):
        matrix, lower, pivots = carry
        column = lax.dynamic_slice_in_dim(matrix, column_index, 1, 1)[:, 0]
        pivot = jnp.sum(jnp.where(positions == column_index, column, 0.0))
        below = jnp.where(positions > column_index, column / pivot, 0.0)
        matrix = matrix - pivot * below[:, None] * below[None, :]
        unit = jnp.where(positions == column_index, 1.0, 0.0)
        lower = lower + (below + unit)[:, None] * unit[None, :]
        pivots = pivots + unit * pivot
        return (matrix, lower, pivots)
    start = (work, jnp.zeros_like(work), jnp.zeros_like(shift))
    matrix, lower, pivots = lax.fori_loop(0, extent, step, start)
    return (lower, pivots)

def to_global(stored):
    width = stored.shape[1]
    return stored.reshape(N_WIDE, R_DEV // PANEL, PANEL, width).transpose(1, 0, 2, 3).reshape(N_WIDE * R_DEV, width)

def to_stored(globe):
    width = globe.shape[1]
    return globe.reshape(R_DEV // PANEL, N_WIDE, PANEL, width).transpose(1, 0, 2, 3).reshape(N_WIDE * R_DEV, width)

def reference(a_rows, xa_panel, za_panel, send_order, recv_order, shift, resident):
    first = jnp.dot(a_rows.astype(jnp.float32), xa_panel.astype(jnp.float32), preferred_element_type=jnp.float32)
    second = jnp.dot(a_rows.astype(jnp.float32), za_panel.astype(jnp.float32), preferred_element_type=jnp.float32)
    schur = first * second
    slot_rows = R_DEV // N_WIDE
    per_device = schur.reshape(N_WIDE, R_DEV, COLS)
    sent = jnp.take_along_axis(per_device, send_order[:, :, None], axis=1)
    buffers = sent.reshape(N_WIDE, N_WIDE, slot_rows, COLS).transpose(1, 0, 2, 3).reshape(N_WIDE, R_DEV, COLS)
    stored = jnp.take_along_axis(buffers, recv_order[:, :, None], axis=1).reshape(N_WIDE * R_DEV, COLS)
    globe = to_global(stored)
    lower, pivots = factor(globe[:PANEL, :PANEL], shift)
    identity = jnp.eye(PANEL, dtype=lower.dtype)
    inverse = lax.linalg.triangular_solve(lower, identity, left_side=True, lower=True, unit_diagonal=True)
    scaled = jnp.dot(globe[:, :PANEL], inverse.T, precision=lax.Precision.HIGHEST)
    panel = jnp.concatenate([lower, (scaled / pivots[None, :])[PANEL:]], axis=0)
    tail = scaled[PANEL:COLS + RES]
    update = jnp.dot(panel, tail.T, precision=lax.Precision.HIGHEST)
    keep = (jnp.arange(N_WIDE * R_DEV) >= PANEL)[:, None]
    formed = globe[:, PANEL:] - jnp.where(keep, update[:, :COLS - PANEL], 0.0)
    factored = to_stored(jnp.concatenate([panel, formed], axis=1))
    resident_glob = to_global(resident).astype(jnp.float32)
    updated = to_stored((resident_glob - jnp.where(keep, update[:, COLS - PANEL:], 0.0)).astype(jnp.bfloat16))
    return (factored, updated, pivots)
```

```python
import functools
import math

import jax
import jax.numpy as jnp
from jax import lax
from jax.experimental import pallas as pl
from jax.experimental.pallas import tpu as pltpu
from jax.sharding import PartitionSpec as P

PANEL = 64
LANES = 128
Q_MAX = 32767.0
F32 = jnp.float32
BF16 = jnp.bfloat16


def lane_iota(shape):
    return lax.broadcasted_iota(jnp.int32, shape, len(shape) - 1)


def exchange_kernel(
    n, n_lead,
    a_hbm, xa_hbm, za_hbm, send_ref, slot_a_ref, slot_b_ref,
    stored_a, stored_b, leading,
    a_vmem, gathered, sa, sr, sb, lead_out, rest_f, rest_out,
    lead_in, rest_in, rest_g, both_a, first_rows, leading_src,
    a_sem, own_sem, ag_send, ag_recv1, ag_recv2, ag_recv3,
    lead_send, lead_recv, rest_send, rest_recv,
    tree_send1, tree_send2, tree_send3, tree_recv1, tree_recv2, tree_recv3,
):
    side = math.isqrt(n // 2)
    rows = a_vmem.shape[0]
    per = rows // n
    pair = per // 2
    me = lax.axis_index("wide")
    core = lax.rem(me, 2)
    chip = lax.div(me, 2)
    x = lax.rem(chip, side)
    y = lax.div(chip, side)
    u = x + core * (y - x)
    v = y + core * (x - y)
    sibling = chip * 2 + 1 - core

    def chip_of(uu, vv):
        return vv * (side - (side - 1) * core) + uu * (1 + (side - 1) * core)

    def wrap(value):
        return lax.rem(value + 2 * side, side)

    def remote(src, dst, send, recv, target):
        pltpu.make_async_remote_copy(
            src_ref=src, dst_ref=dst, send_sem=send, recv_sem=recv,
            device_id={"wide": target}, device_id_type=pl.DeviceIdType.MESH,
        ).start()

    def await_bytes(ref, sem):
        pltpu.make_async_copy(ref, ref, sem).wait()

    a_copy = pltpu.make_async_copy(a_hbm, a_vmem, a_sem)
    a_copy.start()
    own_x = pltpu.make_async_copy(xa_hbm, gathered.at[chip, core, 0], own_sem.at[0])
    own_z = pltpu.make_async_copy(za_hbm, gathered.at[chip, core, 1], own_sem.at[1])
    own_x.start()
    own_z.start()

    barrier = pltpu.get_barrier_semaphore()
    partners = [chip_of(wrap(u + i), v) * 2 + core for i in range(1, side)]
    partners += [chip_of(u, wrap(v + d)) * 2 + core for d in (1, -1)]
    partners += [sibling]
    for partner in partners:
        pl.semaphore_signal(
            barrier, inc=1, device_id={"wide": partner}, device_id_type=pl.DeviceIdType.MESH
        )
    rest_f[:, 3 * pair :, :] = jnp.zeros((n, 16 - 3 * pair, LANES), F32)
    own_x.wait()
    own_z.wait()
    pl.semaphore_wait(barrier, len(partners))

    def send_block(block_chip, target, send, recv):
        block = gathered.at[block_chip, core]
        remote(block, block, send, recv, target)

    half = side // 2
    for i in sorted(range(1, side), key=lambda i: -min(i, side - i)):
        send_block(chip, chip_of(wrap(u + i), v) * 2 + core, ag_send.at[0], ag_recv1)
    await_bytes(gathered.at[0 : side - 1, 0], ag_recv1)
    for step in range(1, half + 2):
        for part in range(2):
            for way, direction in enumerate((1, -1)):
                last_ok = part == way
                if step == half + 1 and not last_ok:
                    continue
                if step > 1:
                    await_bytes(gathered.at[0:half, 0], ag_recv2.at[way, step - 2, part])
                row = wrap(v - direction * (step - 1))
                blocks = [chip_of(part * half + k, row) for k in range(half)]
                if step < half or (step == half and last_ok):
                    target = chip_of(u, wrap(v + direction)) * 2 + core
                    for block in blocks:
                        send_block(block, target, ag_send.at[1], ag_recv2.at[way, step - 1, part])
                if step > 1 or way == 0:
                    for block in blocks:
                        send_block(block, sibling, ag_send.at[2], ag_recv3)
    await_bytes(gathered.at[:, 0], ag_recv3)
    a_copy.wait()

    tile = rows // 4
    depth = a_vmem.shape[1]

    def product(t, _):
        at = pl.ds(pl.multiple_of(t * tile, tile), tile)
        lhs = a_vmem[at, :]
        cols = gathered.shape[-1]
        one = jnp.dot(lhs, gathered[:, :, 0].reshape(depth, cols), preferred_element_type=F32)
        two = jnp.dot(lhs, gathered[:, :, 1].reshape(depth, cols), preferred_element_type=F32)
        schur = one * two
        sa[at, :] = schur[:, :LANES]
        sr[at, :] = pltpu.roll(schur[:, :LANES], PANEL, 1)
        sb[at, :] = schur[:, LANES:]
        return 0

    lax.fori_loop(0, 4, product, 0)

    low = lane_iota((1, LANES)) < PANEL

    def pack_lead(e, _):
        for k in range(pair):
            one = send_ref[0, e * per + k]
            two = send_ref[0, e * per + pair + k]
            lead_out[e, pl.ds(k, 1), :] = jnp.where(
                low, sa[pl.ds(one, 1), :], sr[pl.ds(two, 1), :]
            )
        return 0

    lax.fori_loop(0, n, pack_lead, 0)

    def send_to(e, source, target_ref, send, recv):
        @pl.when(e != me)
        def _():
            remote(source.at[e], target_ref.at[me], send, recv, e)

    def lead_first(i, _):
        send_to(lax.rem(me + i, n_lead), lead_out, lead_in, lead_send, lead_recv)
        return 0

    def lead_other(i, _):
        e = n_lead + lax.rem(me + i, n - n_lead)
        send_to(e, lead_out, lead_in, lead_send, lead_recv)
        return 0

    lax.fori_loop(0, n_lead, lead_first, 0)
    lax.fori_loop(0, n - n_lead, lead_other, 0)
    lead_in[me] = lead_out[me]

    def pack_rest(e, _):
        for k in range(pair):
            one = send_ref[0, e * per + k]
            two = send_ref[0, e * per + pair + k]
            rest_f[e, pl.ds(k, 1), :] = sb[pl.ds(one, 1), :]
            rest_f[e, pl.ds(pair + k, 1), :] = sb[pl.ds(two, 1), :]
            rest_f[e, pl.ds(2 * pair + k, 1), :] = jnp.where(
                low, sr[pl.ds(one, 1), :], sa[pl.ds(two, 1), :]
            )
        return 0

    lax.fori_loop(0, n, pack_rest, 0)

    def quantize(i, _):
        at = pl.ds(i * 8, 8)
        values = rest_f[at]
        largest = jnp.max(jnp.abs(values), axis=1, keepdims=True)
        power = jnp.floor(jnp.log2(jnp.maximum(largest, 1e-30))) + 1.0
        scale = Q_MAX / jnp.exp2(power)
        coded = jnp.clip(jnp.round(values * scale), -Q_MAX, Q_MAX)
        spot = lax.broadcasted_iota(jnp.int32, values.shape, 1)
        coded = jnp.where(spot == 3 * pair, power, coded)
        rest_out[at] = coded.astype(jnp.int32).astype(jnp.int16)
        return 0

    lax.fori_loop(0, n // 8, quantize, 0)

    await_bytes(lead_in.at[0 : n - 1], lead_recv)

    def spread_lead(i, _):
        at = pl.ds(i * 8, 8)
        values = lead_in[at]
        both_a[0, at, 0:pair] = values
        both_a[1, at, 0:pair] = pltpu.roll(values, PANEL, 2)
        return 0

    lax.fori_loop(0, n // 8, spread_lead, 0)
    flat_a = both_a.reshape(2 * n * 8, LANES)

    def first(q, _):
        first_rows[pl.ds(q, 1), :] = flat_a[pl.ds(slot_a_ref[0, q], 1), :]
        return 0

    lax.fori_loop(0, PANEL, first, 0)
    hp = PANEL // 2
    leading_src[...] = jnp.where(
        low, first_rows[0:hp, :], pltpu.roll(first_rows[hp:PANEL, :], PANEL, 1)
    )

    group = 2 * side
    levels = -(-n_lead // group)

    @pl.when(me < n_lead)
    def _():
        leading[me] = leading_src[...]
        for i in range(1, side):
            target = (wrap(y + i) * side + x) * 2 + core
            remote(leading_src, leading.at[me], tree_send1, tree_recv1.at[y], target)

    for m in range(levels):
        e = m * group + 2 * x + core

        @pl.when(e < n_lead)
        def _(m=m, e=e):
            @pl.when(y != m)
            def _():
                await_bytes(leading.at[0], tree_recv1.at[m])

            for i in range(1, side):
                target = (y * side + wrap(x + i)) * 2 + core
                remote(leading.at[e], leading.at[e], tree_send2.at[m], tree_recv2.at[e], target)
            remote(leading.at[e], leading.at[e], tree_send3.at[e], tree_recv3.at[e], sibling)

    def rest_all(i, _):
        send_to(lax.rem(me + i, n), rest_out, rest_in, rest_send, rest_recv)
        return 0

    lax.fori_loop(1, n, rest_all, 0)
    rest_in[me] = rest_out[me]

    for m in range(levels):
        for i in range(1, side):
            e = m * group + 2 * wrap(x + i) + core

            @pl.when(e < n_lead)
            def _(e=e):
                await_bytes(leading.at[0], tree_recv2.at[e])
                remote(leading.at[e], leading.at[e], tree_send3.at[e], tree_recv3.at[e], sibling)

    def from_sibling(e, _):
        @pl.when(lax.rem(e, 2) != core)
        def _():
            await_bytes(leading.at[0], tree_recv3.at[e])

        return 0

    lax.fori_loop(0, n_lead, from_sibling, 0)

    await_bytes(rest_in.at[0 : n - 1], rest_recv)

    def spread_rest(i, _):
        at = pl.ds(i * 8, 8)
        coded = rest_in[at].astype(jnp.int32).astype(F32)
        power = coded[:, 3 * pair : 3 * pair + 1]
        values = coded * (jnp.exp2(power) / Q_MAX)
        rest_g[at] = values
        mid = values[:, 2 * pair : 3 * pair]
        kept = lane_iota(mid.shape) < PANEL
        both_a[0, at, 0:pair] = jnp.where(kept, both_a[0, at, 0:pair], pltpu.roll(mid, PANEL, 2))
        both_a[1, at, 0:pair] = jnp.where(kept, both_a[1, at, 0:pair], mid)
        return 0

    lax.fori_loop(0, n // 8, spread_rest, 0)
    flat_b = rest_g.reshape(n * 16, LANES)

    def place(i, _):
        for k in range(8):
            q = i * 8 + k
            stored_a[pl.ds(q, 1), :] = flat_a[pl.ds(slot_a_ref[0, q], 1), :]
            stored_b[pl.ds(q, 1), :] = flat_b[pl.ds(slot_b_ref[0, q], 1), :]
        return 0

    lax.fori_loop(0, rows // 8, place, 0)

    await_bytes(gathered.at[0 : side - 1, 0], ag_send.at[0])
    await_bytes(gathered.at[0 : side * (side - 1), 0], ag_send.at[1])
    await_bytes(gathered.at[:, 0], ag_send.at[2])
    await_bytes(lead_out.at[0 : n - 1], lead_send)
    await_bytes(rest_out.at[0 : n - 1], rest_send)

    @pl.when(me < n_lead)
    def _():
        await_bytes(leading.at[0 : side - 1], tree_send1)

    for m in range(levels):
        e = m * group + 2 * x + core

        @pl.when(e < n_lead)
        def _(m=m):
            await_bytes(leading.at[0 : side - 1], tree_send2.at[m])

    def to_sibling(e, _):
        @pl.when(lax.rem(e, 2) == core)
        def _():
            await_bytes(leading.at[0], tree_send3.at[e])

        return 0

    lax.fori_loop(0, n_lead, to_sibling, 0)


def exchange(n, n_lead, a_rows, xa, za, send_order, slot_a, slot_b):
    rows, depth = a_rows.shape
    cols = xa.shape[1]
    share = xa.shape[0]
    per = rows // n
    pair = per // 2
    side = math.isqrt(n // 2)
    hp = PANEL // 2
    dma = pltpu.SemaphoreType.DMA
    any_spec = pl.BlockSpec(memory_space=pl.ANY)
    smem = pl.BlockSpec(memory_space=pltpu.SMEM)
    vmem = pl.BlockSpec(memory_space=pltpu.VMEM)
    levels = -(-n_lead // (2 * side))
    return pl.pallas_call(
        functools.partial(exchange_kernel, n, n_lead),
        out_shape=(
            jax.ShapeDtypeStruct((rows, LANES), F32),
            jax.ShapeDtypeStruct((rows, LANES), F32),
            jax.ShapeDtypeStruct((n_lead, hp, LANES), F32),
        ),
        in_specs=[any_spec, any_spec, any_spec, smem, smem, smem],
        out_specs=(vmem, vmem, vmem),
        scratch_shapes=[
            pltpu.VMEM((rows, depth), BF16),
            pltpu.VMEM((n // 2, 2, 2, share, cols), BF16),
            pltpu.VMEM((rows, LANES), F32),
            pltpu.VMEM((rows, LANES), F32),
            pltpu.VMEM((rows, LANES), F32),
            pltpu.VMEM((n, pair, LANES), F32),
            pltpu.VMEM((n, 16, LANES), F32),
            pltpu.VMEM((n, 16, LANES), jnp.int16),
            pltpu.VMEM((n, pair, LANES), F32),
            pltpu.VMEM((n, 16, LANES), jnp.int16),
            pltpu.VMEM((n, 16, LANES), F32),
            pltpu.VMEM((2, n, 8, LANES), F32),
            pltpu.VMEM((PANEL, LANES), F32),
            pltpu.VMEM((hp, LANES), F32),
            dma, dma((2,)), dma((3,)), dma, dma((2, side // 2, 2)), dma,
            dma, dma, dma, dma,
            dma, dma((levels,)), dma((n_lead,)), dma((side,)), dma((n_lead,)), dma((n_lead,)),
        ],
        compiler_params=pltpu.CompilerParams(
            collective_id=0, has_side_effects=True, vmem_limit_bytes=48 * 1024 * 1024
        ),
    )(a_rows, xa, za, send_order, slot_a, slot_b)


def two_parts(values):
    high = values.astype(BF16)
    return high, (values - high.astype(F32)).astype(BF16)


def left_stack(twice):
    high, mid = two_parts(twice)
    return jnp.concatenate([high, mid], axis=1)


def right_stack(twice):
    high, mid = two_parts(twice)
    once = jnp.where(lane_iota(twice.shape) < PANEL, high.astype(F32), mid.astype(F32))
    once = once.astype(BF16)
    return jnp.concatenate([once, once], axis=1)


def dot_nt(a, b):
    return lax.dot_general(a, b, (((1,), (1,)), ((), ())), preferred_element_type=F32)


def finish_kernel(
    a_ref, b_ref, leading, shift_ref, resident_ref,
    factored_ref, updated_ref, pivots_ref,
    work, lower_ref, inverse_ref, tail_ref,
):
    step = pl.program_id(0)
    me = lax.axis_index("wide")
    tile = a_ref.shape[0]

    @pl.when(step == 0)
    def _():
        head = leading[0]
        lanes = lane_iota(head.shape)
        turned = pltpu.roll(head, PANEL, 1)
        block = jnp.concatenate([head, turned], axis=0)
        r = lax.broadcasted_iota(jnp.int32, block.shape, 0)
        c = lane_iota(block.shape)
        inside = c < PANEL
        strict = jnp.where((r > c) & inside, block, 0.0)
        pad = jnp.concatenate([strict, jnp.zeros_like(strict)], axis=0)
        mirrored = jnp.where((r >= c) & inside, block, 0.0) + pad.T[:PANEL, :]
        magnitude = jnp.sum(jnp.abs(mirrored), axis=0, keepdims=True)
        diagonal = magnitude + shift_ref[...]
        start = jnp.where(r == c, diagonal, mirrored)
        work[...] = jnp.where(inside, start, jnp.where(r == c - PANEL, 1.0, 0.0))
        lower_ref[...] = jnp.zeros_like(block)

        def eliminate(j, pivots):
            matrix = work[...]
            row = work[pl.ds(j, 1), :]
            column = jnp.sum(jnp.where(c == j, matrix, 0.0), axis=1, keepdims=True)
            first = lane_iota(row.shape) == j
            pivot = jnp.sum(jnp.where(first, row, 0.0), axis=1, keepdims=True)
            below = jnp.where(r > j, column / pivot, 0.0)
            work[...] = matrix - below * row
            lower_ref[...] += jnp.where(c == j, below + jnp.where(r == j, 1.0, 0.0), 0.0)
            return jnp.where(first, pivot, pivots)

        pivots = lax.fori_loop(0, PANEL, eliminate, jnp.ones((1, LANES), F32))
        pivots_ref[...] = pivots
        final = work[...]
        inverse = jnp.where(inside, pltpu.roll(final, PANEL, 1), final)
        inverse_ref[0:PANEL, :] = right_stack(inverse)
        inverse_ref[PANEL:, :] = jnp.zeros_like(inverse_ref[PANEL:, :])
        blocks = leading[...]
        keep = lane_iota(blocks.shape) < PANEL
        other = pltpu.roll(blocks, PANEL, 2)
        top = jnp.where(keep, blocks, other)
        bottom = jnp.where(keep, other, blocks)
        full = jnp.concatenate([top, bottom], axis=1)
        full = full.reshape(full.shape[0] * PANEL, LANES)
        tail = dot_nt(left_stack(full), inverse_ref[...])
        tail = tail + pltpu.roll(tail, PANEL, 1)
        place = lax.broadcasted_iota(jnp.int32, tail.shape, 0)
        tail_ref[...] = right_stack(jnp.where(place < PANEL, 0.0, tail))

    a = a_ref[...]
    lanes = lane_iota(a.shape)
    local = lax.broadcasted_iota(jnp.int32, a.shape, 0) + step * tile
    low = lanes < PANEL
    lead = jnp.where(low, a, pltpu.roll(a, PANEL, 1))
    scaled = dot_nt(left_stack(lead), inverse_ref[...])
    panel = scaled / pivots_ref[...]
    is_top = (local < PANEL) & (me == 0)
    fill = tile // PANEL
    lower = jnp.concatenate([lower_ref[...]] * fill, axis=0)
    panel = jnp.where(is_top, lower, panel)
    update = dot_nt(left_stack(panel + pltpu.roll(panel, PANEL, 1)), tail_ref[...])
    cols = b_ref.shape[1] + a.shape[1]

    def kept(values):
        rows_at = lax.broadcasted_iota(jnp.int32, values.shape, 0) + step * tile
        return jnp.where((rows_at < PANEL) & (me == 0), 0.0, values)

    factored_ref[:, :LANES] = jnp.where(low, panel, a - kept(update[:, :LANES]))
    factored_ref[:, LANES:] = b_ref[...] - kept(update[:, LANES:cols])
    updated_ref[...] = (resident_ref[...].astype(F32) - kept(update[:, cols:])).astype(BF16)


def finish(stored_a, stored_b, leading, shift, resident):
    rows = stored_a.shape[0]
    tile = 256
    width = resident.shape[1]
    cols = stored_a.shape[1] + stored_b.shape[1]
    n_lead = leading.shape[0]
    row_spec = lambda w: pl.BlockSpec((tile, w), lambda i: (i, 0))
    whole = lambda shape: pl.BlockSpec(shape, lambda i: (0,) * len(shape))
    return pl.pallas_call(
        finish_kernel,
        grid=(rows // tile,),
        out_shape=(
            jax.ShapeDtypeStruct((rows, cols), F32),
            jax.ShapeDtypeStruct((rows, width), BF16),
            jax.ShapeDtypeStruct((1, LANES), F32),
        ),
        in_specs=[
            row_spec(LANES), row_spec(LANES), whole(leading.shape), whole((1, LANES)),
            row_spec(width),
        ],
        out_specs=(row_spec(cols), row_spec(width), whole((1, LANES))),
        scratch_shapes=[
            pltpu.VMEM((PANEL, LANES), F32),
            pltpu.VMEM((PANEL, LANES), F32),
            pltpu.VMEM((LANES, 2 * LANES), BF16),
            pltpu.VMEM((n_lead * PANEL, 2 * LANES), BF16),
        ],
        compiler_params=pltpu.CompilerParams(vmem_limit_bytes=32 * 1024 * 1024),
    )(stored_a, stored_b, leading, shift, resident)


def on_device(n, a_rows, xa_panel, za_panel, send_order, recv_order, shift, resident):
    rows = a_rows.shape[0]
    per = rows // n
    pair = per // 2
    needed = xa_panel.shape[1] + resident.shape[1]
    n_lead = -(-needed // PANEL)
    source = recv_order // per
    slot = recv_order % per
    slot_a = (slot // pair) * (n * 8) + source * 8 + slot % pair
    slot_b = source * 16 + slot
    stored_a, stored_b, leading = exchange(
        n, n_lead, a_rows, xa_panel, za_panel, send_order, slot_a, slot_b
    )
    padded = jnp.concatenate([shift, jnp.ones_like(shift)])[None, :]
    factored, updated, pivots = finish(stored_a, stored_b, leading, padded, resident)
    return factored, updated, pivots[0, :PANEL]


def solution(mesh):
    spread = P(("parts", "wide"), None)
    return jax.shard_map(
        functools.partial(on_device, mesh.shape["wide"]),
        mesh=mesh,
        in_specs=(spread, spread, spread, spread, spread, P("parts"), spread),
        out_specs=(spread, spread, P("parts")),
        check_vma=False,
    )
```

```python
import functools
import math

import jax
import jax.numpy as jnp
from jax import lax
from jax.experimental import pallas as pl
from jax.experimental.pallas import tpu as pltpu
from jax.sharding import PartitionSpec as P

PANEL = 64
LANES = 128
Q_MAX = 32767.0
F32 = jnp.float32
BF16 = jnp.bfloat16


def lane_iota(shape):
    return lax.broadcasted_iota(jnp.int32, shape, len(shape) - 1)


def u_groups(side):
    half = side // 2
    groups = [(0,)] + [(o, -o) for o in range(1, half - 1)]
    return groups + [(half - 1, 1 - half, half)]


def exchange_kernel(
    n, n_lead,
    a_hbm, xa_hbm, za_hbm, send_hbm, recv_hbm, shift_hbm,
    stored_a, stored_b, leading, work, lower_ref, pivots_ref,
    a_vmem, gathered, sa, sr, sb, lead_out, rest_f, rest_out,
    lead_in, rest_in, rest_g, both_a, first_rows, leading_src,
    shift_ref, send_ref, recv_ref, slots,
    a_sem, own_sem, order_sem, ag_send, ag_recv_u, ag_recv_v, ag_recv_s,
    lead_send, lead_recv, rest_send, rest_recv,
    tree_send1, tree_send2, tree_send3, tree_recv1, tree_recv2, tree_recv3,
):
    side = math.isqrt(n // 2)
    rows = a_vmem.shape[0]
    per = rows // n
    pair = per // 2
    me = lax.axis_index("wide")
    core = lax.rem(me, 2)
    chip = lax.div(me, 2)
    x = lax.rem(chip, side)
    y = lax.div(chip, side)
    u = x + core * (y - x)
    v = y + core * (x - y)
    sibling = chip * 2 + 1 - core
    step_u = 1 + (side - 1) * core
    step_v = side - (side - 1) * core

    def chip_of(uu, vv):
        return vv * step_v + uu * step_u

    def wrap(value):
        return lax.rem(value + 2 * side, side)

    def remote(src, dst, send, recv, target):
        pltpu.make_async_remote_copy(
            src_ref=src, dst_ref=dst, send_sem=send, recv_sem=recv,
            device_id={"wide": target}, device_id_type=pl.DeviceIdType.MESH,
        ).start()

    def await_bytes(ref, sem):
        pltpu.make_async_copy(ref, ref, sem).wait()

    own_x = pltpu.make_async_copy(xa_hbm, gathered.at[chip, core, 0], own_sem.at[0])
    own_z = pltpu.make_async_copy(za_hbm, gathered.at[chip, core, 1], own_sem.at[1])
    own_x.start()
    own_z.start()

    at_u = {o: wrap(u + o) for o in range(-(side // 2) + 1, side // 2 + 1)}
    at_v = {o: wrap(v + o) for o in range(-2, 3)}
    to_u = {o: chip_of(at_u[o], v) * 2 + core for o in at_u if o}
    to_v = {o: chip_of(u, at_v[o]) * 2 + core for o in at_v if o}
    barrier = pltpu.get_barrier_semaphore()
    partners = list(to_u.values()) + list(to_v.values()) + [sibling]
    for partner in partners:
        pl.semaphore_signal(
            barrier, inc=1, device_id={"wide": partner}, device_id_type=pl.DeviceIdType.MESH
        )
    a_copy = pltpu.make_async_copy(a_hbm, a_vmem, a_sem)
    send_copy = pltpu.make_async_copy(send_hbm, send_ref, order_sem.at[0])
    recv_copy = pltpu.make_async_copy(recv_hbm, recv_ref, order_sem.at[1])
    a_copy.start()
    send_copy.start()
    shift_copy = pltpu.make_async_copy(shift_hbm, shift_ref, order_sem.at[2])
    recv_copy.start()
    shift_copy.start()
    own_x.wait()
    own_z.wait()
    pl.semaphore_wait(barrier, len(partners))

    def send_block(block_chip, target, send, recv):
        block = gathered.at[block_chip, core]
        remote(block, block, send, recv, target)

    half = side // 2
    groups = u_groups(side)
    group_of = {o: g for g, members in enumerate(groups) for o in members}
    across = ((0, len(groups) - 1), tuple(range(1, len(groups) - 1)))
    signs = (1, -1)
    for o in sorted(to_u, key=lambda o: -abs(o)):
        send_block(chip, to_u[o], ag_send.at[0], ag_recv_u.at[group_of[o]])

    def blocks_of(g, row):
        return [chip_of(at_u[o], row) for o in groups[g]]

    def send_v(g, row, hop, way, jump):
        for block in blocks_of(g, row):
            send_block(
                block, to_v[signs[way] * jump], ag_send.at[1], ag_recv_v.at[way, hop - 1, g]
            )

    def share(g, row):
        for block in blocks_of(g, row):
            send_block(block, sibling, ag_send.at[2], ag_recv_s)

    def arrived(g, hop, way):
        await_bytes(gathered.at[0 : len(groups[g]), 0], ag_recv_v.at[way, hop - 1, g])

    for g in range(len(groups)):
        if g > 0:
            await_bytes(gathered.at[0 : len(groups[g]), 0], ag_recv_u.at[g])
        for jump in (2, 1):
            for way in range(2):
                send_v(g, v, jump, way, jump)
        share(g, v)
    for g in range(len(groups)):
        for way in range(2):
            arrived(g, 2, way)
            row = at_v[-2 * signs[way]]
            if g in across[way]:
                send_v(g, row, 4, way, 2)
            send_v(g, row, 3, way, 1)
            share(g, row)
        for way in range(2):
            arrived(g, 1, way)
            share(g, at_v[-signs[way]])
    for g in range(len(groups)):
        for way in range(2):
            arrived(g, 3, way)
            share(g, wrap(v - 3 * signs[way]))
            if g in across[way]:
                arrived(g, 4, way)
                share(g, wrap(v - 4 * signs[way]))
    a_copy.wait()
    send_copy.wait()
    recv_copy.wait()
    shift_copy.wait()
    await_bytes(gathered.at[:, 0], ag_recv_s)

    tile = rows // 4
    depth = a_vmem.shape[1]

    def product(t, _):
        at = pl.ds(pl.multiple_of(t * tile, tile), tile)
        lhs = a_vmem[at, :]
        cols = gathered.shape[-1]
        one = jnp.dot(lhs, gathered[:, :, 0].reshape(depth, cols), preferred_element_type=F32)
        two = jnp.dot(lhs, gathered[:, :, 1].reshape(depth, cols), preferred_element_type=F32)
        schur = one * two
        sa[at, :] = schur[:, :LANES]
        sr[at, :] = pltpu.roll(schur[:, :LANES], PANEL, 1)
        sb[at, :] = schur[:, LANES:]
        return 0

    lax.fori_loop(0, 4, product, 0)

    low = lane_iota((1, LANES)) < PANEL

    def pack_lead(e, _):
        firsts, seconds = [], []
        for k in range(pair):
            firsts.append(sa[pl.ds(send_ref[0, e * per + k], 1), :])
            seconds.append(sr[pl.ds(send_ref[0, e * per + pair + k], 1), :])
        for k in range(pair):
            lead_out[e, pl.ds(k, 1), :] = jnp.where(low, firsts[k], seconds[k])
        return 0

    def send_to(e, source, target_ref, send, recv):
        @pl.when(e != me)
        def _():
            remote(source.at[e], target_ref.at[me], send, recv, e)

    def turn(start, i, span):
        e = start + i
        return jnp.where(e >= span, e - span, e)

    start_lead = lax.rem(me, n_lead)
    start_other = lax.rem(me, n - n_lead)

    def lead_first(i, _):
        send_to(turn(start_lead, i, n_lead), lead_out, lead_in, lead_send, lead_recv)
        return 0

    def lead_other(i, _):
        e = n_lead + turn(start_other, i, n - n_lead)
        send_to(e, lead_out, lead_in, lead_send, lead_recv)
        return 0

    ahead = min(2 * n_lead, n)
    lax.fori_loop(0, ahead, pack_lead, 0)
    lax.fori_loop(0, n_lead, lead_first, 0)
    lax.fori_loop(ahead, n, pack_lead, 0)
    lax.fori_loop(0, n - n_lead, lead_other, 0)
    lead_in[me] = lead_out[me]

    def pack_rest(e, _):
        parts = []
        for k in range(pair):
            one = send_ref[0, e * per + k]
            two = send_ref[0, e * per + pair + k]
            parts.append((
                sb[pl.ds(one, 1), :], sb[pl.ds(two, 1), :],
                sr[pl.ds(one, 1), :], sa[pl.ds(two, 1), :],
            ))
        for k in range(pair):
            one, two, left, right = parts[k]
            rest_f[e, pl.ds(k, 1), :] = one
            rest_f[e, pl.ds(pair + k, 1), :] = two
            rest_f[e, pl.ds(2 * pair + k, 1), :] = jnp.where(low, left, right)
        return 0

    rest_f[:, 3 * pair :, :] = jnp.zeros((n, 16 - 3 * pair, LANES), F32)
    lax.fori_loop(0, n, pack_rest, 0)

    def quantize(i, _):
        at = pl.ds(i * 8, 8)
        values = rest_f[at]
        largest = jnp.max(jnp.abs(values), axis=1, keepdims=True)
        power = jnp.floor(jnp.log2(jnp.maximum(largest, 1e-30))) + 1.0
        scale = Q_MAX / jnp.exp2(power)
        coded = jnp.clip(jnp.round(values * scale), -Q_MAX, Q_MAX)
        spot = lax.broadcasted_iota(jnp.int32, values.shape, 1)
        coded = jnp.where(spot == 3 * pair, power, coded)
        rest_out[at] = coded.astype(jnp.int32).astype(jnp.int16)
        return 0

    lax.fori_loop(0, n // 8, quantize, 0)

    chunks = 8
    span = n // chunks
    my_chunk = lax.div(me, span)

    def send_rest(i, _):
        send_to(turn(me, i, n), rest_out, rest_in, rest_send, rest_recv.at[my_chunk])
        return 0

    relays_first = (me < n_lead) | ((x == 0) & (core == 0))

    @pl.when(jnp.logical_not(relays_first))
    def _():
        lax.fori_loop(1, n, send_rest, 0)

    magic = -(-65536 // per)
    assert all((j * magic) >> 16 == j // per for j in range(rows))

    def find_slots(i, _):
        for k in range(8):
            slot = recv_ref[0, i * 8 + k]
            source = lax.shift_right_logical(slot * magic, 16)
            slots[0, i * 8 + k] = slot + (16 - per) * source
        return 0


    flat_a = both_a.reshape(n * 16, LANES)
    flat_b = rest_g.reshape(n * 16, LANES)

    def take(source, start):
        return jnp.concatenate(
            [source[pl.ds(slots[0, start + k], 1), :] for k in range(8)], axis=0
        )

    def take_leads():
        await_bytes(lead_in.at[0 : n - 1], lead_recv)

        def spread_lead(i, _):
            at = pl.ds(i * 8, 8)
            values = lead_in[at]
            both_a[at, 0:pair] = values
            both_a[at, pair : 2 * pair] = pltpu.roll(values, PANEL, 2)
            return 0

        lax.fori_loop(0, n // 8, spread_lead, 0)

    hp = PANEL // 2
    group = 2 * side
    levels = -(-n_lead // group)

    @pl.when(me < n_lead)
    def _():
        lax.fori_loop(0, PANEL // 8, find_slots, 0)
        take_leads()

        def first(i, _):
            first_rows[pl.ds(pl.multiple_of(i * 8, 8), 8), :] = take(flat_a, i * 8)
            return 0

        lax.fori_loop(0, PANEL // 8, first, 0)
        packed = jnp.where(
            low, first_rows[0:hp, :], pltpu.roll(first_rows[hp:PANEL, :], PANEL, 1)
        )
        leading_src[...] = packed
        leading[me] = packed
        for i in sorted(range(1, side), key=lambda i: -min(i, side - i)):
            target = (wrap(y + i) * side + x) * 2 + core
            remote(leading_src, leading.at[me], tree_send1, tree_recv1.at[y], target)

    def relay(m, e):
        @pl.when(y != m)
        def _():
            await_bytes(leading.at[0], tree_recv1.at[m])

        for i in sorted(range(1, side), key=lambda i: -min(i, side - i)):
            target = (y * side + wrap(x + i)) * 2 + core
            remote(leading.at[e], leading.at[e], tree_send2.at[m], tree_recv2.at[e], target)
        remote(leading.at[e], leading.at[e], tree_send3.at[e], tree_recv3.at[e], sibling)

    @pl.when((x == 0) & (core == 0))
    def _():
        relay(0, 0)

    @pl.when(relays_first)
    def _():
        lax.fori_loop(1, n, send_rest, 0)

    rest_in[me] = rest_out[me]

    for m in range(levels):
        e = m * group + 2 * x + core

        @pl.when((e < n_lead) & (e > 0))
        def _(m=m, e=e):
            relay(m, e)

    lax.fori_loop(0, rows // 8, find_slots, 0)

    @pl.when(me >= n_lead)
    def _():
        take_leads()

    def pass_on(e):
        await_bytes(leading.at[0], tree_recv2.at[e])
        remote(leading.at[e], leading.at[e], tree_send3.at[e], tree_recv3.at[e], sibling)

    @pl.when((x != 0) & (core == 0))
    def _():
        pass_on(0)

    @pl.when(core == 1)
    def _():
        await_bytes(leading.at[0], tree_recv3.at[0])

    eliminate_block(leading[0], shift_ref, work, lower_ref, pivots_ref)

    for m in range(levels):
        for i in range(1, side):
            e = m * group + 2 * wrap(x + i) + core

            @pl.when((e < n_lead) & (e > 0))
            def _(e=e):
                pass_on(e)

    def from_sibling(e, _):
        @pl.when(lax.rem(e, 2) != core)
        def _():
            await_bytes(leading.at[0], tree_recv3.at[e])

        return 0

    lax.fori_loop(1, n_lead, from_sibling, 0)

    def spread_rest(i, _):
        at = pl.ds(i * 8, 8)
        coded = rest_in[at].astype(jnp.int32).astype(F32)
        power = coded[:, 3 * pair : 3 * pair + 1]
        values = coded * (jnp.exp2(power) / Q_MAX)
        rest_g[at] = values
        mid = values[:, 2 * pair : 3 * pair]
        kept = lane_iota(mid.shape) < PANEL
        both_a[at, 0:pair] = jnp.where(kept, both_a[at, 0:pair], pltpu.roll(mid, PANEL, 2))
        both_a[at, pair : 2 * pair] = jnp.where(kept, both_a[at, pair : 2 * pair], mid)
        return 0

    for chunk in range(chunks):
        at = chunk * span

        @pl.when(my_chunk == chunk)
        def _(chunk=chunk, at=at):
            await_bytes(rest_in.at[at : at + span - 1], rest_recv.at[chunk])

        @pl.when(my_chunk != chunk)
        def _(chunk=chunk, at=at):
            await_bytes(rest_in.at[at : at + span], rest_recv.at[chunk])

        lax.fori_loop(at // 8, (at + span) // 8, spread_rest, 0)

    def place(i, _):
        at = pl.ds(pl.multiple_of(i * 8, 8), 8)
        stored_a[at, :] = take(flat_a, i * 8)
        stored_b[at, :] = take(flat_b, i * 8)
        return 0

    lax.fori_loop(0, rows // 8, place, 0)

    await_bytes(gathered.at[0 : side - 1, 0], ag_send.at[0])
    await_bytes(gathered.at[0 : side * (side - 1), 0], ag_send.at[1])
    await_bytes(gathered.at[:, 0], ag_send.at[2])
    await_bytes(lead_out.at[0 : n - 1], lead_send)
    await_bytes(rest_out.at[0 : n - 1], rest_send)

    @pl.when(me < n_lead)
    def _():
        await_bytes(leading.at[0 : side - 1], tree_send1)

    for m in range(levels):
        e = m * group + 2 * x + core

        @pl.when(e < n_lead)
        def _(m=m):
            await_bytes(leading.at[0 : side - 1], tree_send2.at[m])

    def to_sibling(e, _):
        @pl.when(lax.rem(e, 2) == core)
        def _():
            await_bytes(leading.at[0], tree_send3.at[e])

        return 0

    lax.fori_loop(0, n_lead, to_sibling, 0)


def eliminate_block(head, shift_ref, work, lower_ref, pivots_ref):
    turned = pltpu.roll(head, PANEL, 1)
    block = jnp.concatenate([head, turned], axis=0)
    r = lax.broadcasted_iota(jnp.int32, block.shape, 0)
    c = lane_iota(block.shape)
    inside = c < PANEL
    strict = jnp.where((r > c) & inside, block, 0.0)
    pad = jnp.concatenate([strict, jnp.zeros_like(strict)], axis=0)
    mirrored = jnp.where((r >= c) & inside, block, 0.0) + pad.T[:PANEL, :]
    magnitude = jnp.sum(jnp.abs(mirrored), axis=0, keepdims=True)
    shift = shift_ref[...].reshape(1, PANEL)
    diagonal = magnitude + jnp.concatenate([shift, shift], axis=1)
    start = jnp.where(r == c, diagonal, mirrored)
    work[...] = jnp.where(inside, start, jnp.where(r == c - PANEL, 1.0, 0.0))
    lower_ref[...] = jnp.zeros_like(block)

    lane = lane_iota((1, LANES))

    def pick(values, mask):
        return jnp.sum(jnp.where(mask, values, 0.0), axis=1, keepdims=True)

    def eliminate(i, pivots):
        j = 2 * i
        matrix = work[...]
        row0 = work[pl.ds(j, 1), :]
        row1 = work[pl.ds(j + 1, 1), :]
        column0 = pick(matrix, c == j)
        column1 = pick(matrix, c == j + 1)
        pivot0 = pick(row0, lane == j)
        beside = pick(row0, lane == j + 1)
        under = pick(row1, lane == j)
        corner = pick(row1, lane == j + 1)
        inverse0 = 1.0 / pivot0
        ratio = under * inverse0
        below0 = jnp.where(r > j, column0 * inverse0, 0.0)
        row1 = row1 - ratio * row0
        pivot1 = corner - ratio * beside
        below1 = jnp.where(r > j + 1, (column1 - below0 * beside) * (1.0 / pivot1), 0.0)
        work[...] = matrix - below0 * row0 - below1 * row1
        new0 = below0 + jnp.where(r == j, 1.0, 0.0)
        new1 = below1 + jnp.where(r == j + 1, 1.0, 0.0)
        lower_ref[...] += jnp.where(c == j, new0, jnp.where(c == j + 1, new1, 0.0))
        return jnp.where(lane == j, pivot0, jnp.where(lane == j + 1, pivot1, pivots))

    pivots_ref[...] = lax.fori_loop(0, PANEL // 2, eliminate, jnp.ones((1, LANES), F32))


def exchange(n, n_lead, a_rows, xa, za, send_order, recv_order, shift):
    rows, depth = a_rows.shape
    cols = xa.shape[1]
    share = xa.shape[0]
    per = rows // n
    pair = per // 2
    side = math.isqrt(n // 2)
    hp = PANEL // 2
    dma = pltpu.SemaphoreType.DMA
    hbm = pl.BlockSpec(memory_space=pltpu.HBM)
    vmem = pl.BlockSpec(memory_space=pltpu.VMEM)
    levels = -(-n_lead // (2 * side))
    n_groups = len(u_groups(side))
    return pl.pallas_call(
        functools.partial(exchange_kernel, n, n_lead),
        out_shape=(
            jax.ShapeDtypeStruct((rows, LANES), F32),
            jax.ShapeDtypeStruct((rows, LANES), F32),
            jax.ShapeDtypeStruct((n_lead, hp, LANES), F32),
            jax.ShapeDtypeStruct((PANEL, LANES), F32),
            jax.ShapeDtypeStruct((PANEL, LANES), F32),
            jax.ShapeDtypeStruct((1, LANES), F32),
        ),
        in_specs=[hbm] * 6,
        out_specs=(vmem,) * 6,
        scratch_shapes=[
            pltpu.VMEM((rows, depth), BF16),
            pltpu.VMEM((n // 2, 2, 2, share, cols), BF16),
            pltpu.VMEM((rows, LANES), F32),
            pltpu.VMEM((rows, LANES), F32),
            pltpu.VMEM((rows, LANES), F32),
            pltpu.VMEM((n, pair, LANES), F32),
            pltpu.VMEM((n, 16, LANES), F32),
            pltpu.VMEM((n, 16, LANES), jnp.int16),
            pltpu.VMEM((n, pair, LANES), F32),
            pltpu.VMEM((n, 16, LANES), jnp.int16),
            pltpu.VMEM((n, 16, LANES), F32),
            pltpu.VMEM((n, 16, LANES), F32),
            pltpu.VMEM((PANEL, LANES), F32),
            pltpu.VMEM((hp, LANES), F32),
            pltpu.VMEM((PANEL,), F32),
            pltpu.SMEM((1, rows), jnp.int32),
            pltpu.SMEM((1, rows), jnp.int32),
            pltpu.SMEM((1, rows), jnp.int32),
            dma, dma((2,)), dma((3,)), dma((3,)), dma((n_groups,)), dma((2, 4, n_groups)), dma,
            dma, dma, dma, dma((8,)),
            dma, dma((levels,)), dma((n_lead,)), dma((side,)), dma((n_lead,)), dma((n_lead,)),
        ],
        compiler_params=pltpu.CompilerParams(
            collective_id=0, has_side_effects=True, vmem_limit_bytes=48 * 1024 * 1024
        ),
    )(*(pltpu.with_memory_space_constraint(o, pltpu.HBM) for o in (
        a_rows, xa, za, send_order, recv_order, shift
    )))


def two_parts(values):
    high = values.astype(BF16)
    return high, (values - high.astype(F32)).astype(BF16)


def left_stack(twice):
    high, mid = two_parts(twice)
    return jnp.concatenate([high, mid], axis=1)


def right_stack(twice):
    high, mid = two_parts(twice)
    once = jnp.where(lane_iota(twice.shape) < PANEL, high.astype(F32), mid.astype(F32))
    once = once.astype(BF16)
    return jnp.concatenate([once, once], axis=1)


def dot_nt(a, b):
    return lax.dot_general(a, b, (((1,), (1,)), ((), ())), preferred_element_type=F32)


def finish_kernel(
    a_ref, b_ref, leading, work, lower_ref, pivot_ref, resident_ref,
    factored_ref, updated_ref, pivots_ref,
    inverse_ref, tail_ref,
):
    step = pl.program_id(0)
    me = lax.axis_index("wide")
    tile = a_ref.shape[0]

    @pl.when(step == 0)
    def _():
        final = work[...]
        inside = lane_iota(final.shape) < PANEL
        pivots_ref[...] = pivot_ref[...][0, :PANEL]
        inverse = jnp.where(inside, pltpu.roll(final, PANEL, 1), final)
        inverse_ref[0:PANEL, :] = right_stack(inverse)
        inverse_ref[PANEL:, :] = jnp.zeros_like(inverse_ref[PANEL:, :])
        blocks = leading[...]
        keep = lane_iota(blocks.shape) < PANEL
        other = pltpu.roll(blocks, PANEL, 2)
        top = jnp.where(keep, blocks, other)
        bottom = jnp.where(keep, other, blocks)
        full = jnp.concatenate([top, bottom], axis=1)
        full = full.reshape(full.shape[0] * PANEL, LANES)
        tail = dot_nt(left_stack(full), inverse_ref[...])
        tail = tail + pltpu.roll(tail, PANEL, 1)
        place = lax.broadcasted_iota(jnp.int32, tail.shape, 0)
        tail_ref[...] = right_stack(jnp.where(place < PANEL, 0.0, tail))

    a = a_ref[...]
    lanes = lane_iota(a.shape)
    local = lax.broadcasted_iota(jnp.int32, a.shape, 0) + step * tile
    low = lanes < PANEL
    lead = jnp.where(low, a, pltpu.roll(a, PANEL, 1))
    scaled = dot_nt(left_stack(lead), inverse_ref[...])
    panel = scaled / pivot_ref[...]
    is_top = (local < PANEL) & (me == 0)
    fill = tile // PANEL
    lower = jnp.concatenate([lower_ref[...]] * fill, axis=0)
    panel = jnp.where(is_top, lower, panel)
    update = dot_nt(left_stack(panel + pltpu.roll(panel, PANEL, 1)), tail_ref[...])
    cols = b_ref.shape[1] + a.shape[1]

    def kept(values):
        rows_at = lax.broadcasted_iota(jnp.int32, values.shape, 0) + step * tile
        return jnp.where((rows_at < PANEL) & (me == 0), 0.0, values)

    factored_ref[:, :LANES] = jnp.where(low, panel, a - kept(update[:, :LANES]))
    factored_ref[:, LANES:] = b_ref[...] - kept(update[:, LANES:cols])
    updated_ref[...] = (resident_ref[...].astype(F32) - kept(update[:, cols:])).astype(BF16)


def finish(stored_a, stored_b, leading, work, lower, pivots, resident):
    rows = stored_a.shape[0]
    tile = 256
    width = resident.shape[1]
    cols = stored_a.shape[1] + stored_b.shape[1]
    n_lead = leading.shape[0]
    row_spec = lambda w: pl.BlockSpec((tile, w), lambda i: (i, 0))
    whole = lambda shape: pl.BlockSpec(shape, lambda i: (0,) * len(shape))
    return pl.pallas_call(
        finish_kernel,
        grid=(rows // tile,),
        out_shape=(
            jax.ShapeDtypeStruct((rows, cols), F32),
            jax.ShapeDtypeStruct((rows, width), BF16),
            jax.ShapeDtypeStruct((PANEL,), F32),
        ),
        in_specs=[
            row_spec(LANES), row_spec(LANES), whole(leading.shape), whole(work.shape),
            whole(lower.shape), whole(pivots.shape), row_spec(width),
        ],
        out_specs=(row_spec(cols), row_spec(width), whole((PANEL,))),
        scratch_shapes=[
            pltpu.VMEM((LANES, 2 * LANES), BF16),
            pltpu.VMEM((n_lead * PANEL, 2 * LANES), BF16),
        ],
        compiler_params=pltpu.CompilerParams(vmem_limit_bytes=32 * 1024 * 1024),
    )(stored_a, stored_b, leading, work, lower, pivots, resident)


def on_device(n, a_rows, xa_panel, za_panel, send_order, recv_order, shift, resident):
    needed = xa_panel.shape[1] + resident.shape[1]
    n_lead = -(-needed // PANEL)
    stored_a, stored_b, leading, work, lower, pivots = exchange(
        n, n_lead, a_rows, xa_panel, za_panel, send_order, recv_order, shift
    )
    return finish(stored_a, stored_b, leading, work, lower, pivots, resident)


def solution(mesh):
    spread = P(("parts", "wide"), None)
    return jax.shard_map(
        functools.partial(on_device, mesh.shape["wide"]),
        mesh=mesh,
        in_specs=(spread, spread, spread, spread, spread, P("parts"), spread),
        out_specs=(spread, spread, P("parts")),
        check_vma=False,
    )
```

```python
import functools
import math

import jax
import jax.numpy as jnp
from jax import lax
from jax.experimental import pallas as pl
from jax.experimental.pallas import tpu as pltpu
from jax.sharding import PartitionSpec as P

PANEL = 64
SPREAD = 45
LANES = 128
Q_MAX = 32767.0
F32 = jnp.float32
BF16 = jnp.bfloat16


def lane_iota(shape):
    return lax.broadcasted_iota(jnp.int32, shape, len(shape) - 1)


def u_groups(side):
    half = side // 2
    groups = [(0,)] + [(o, -o) for o in range(1, half - 1)]
    return groups + [(half - 1, 1 - half, half)]


def exchange_kernel(
    n, n_lead,
    a_hbm, xa_hbm, za_hbm, send_hbm, recv_hbm, shift_hbm,
    stored_a, stored_b, leading, work, lower_ref, pivots_ref,
    a_vmem, gathered, sa, sr, sb, lead_out, rest_f, rest_out,
    lead_in, rest_in, rest_g, both_a, first_rows, leading_src,
    shift_ref, send_ref, recv_ref, slots,
    a_sem, own_sem, order_sem, ag_send, ag_recv_u, ag_recv_v, ag_recv_s,
    lead_send, lead_recv, rest_send, rest_recv,
    tree_send1, tree_send2, tree_send3, tree_recv1, tree_recv2, tree_recv3,
):
    side = math.isqrt(n // 2)
    rows = a_vmem.shape[0]
    per = rows // n
    pair = per // 2
    me = lax.axis_index("wide")
    core = lax.rem(me, 2)
    chip = lax.div(me, 2)
    x = lax.rem(chip, side)
    y = lax.div(chip, side)
    u = x + core * (y - x)
    v = y + core * (x - y)
    sibling = chip * 2 + 1 - core
    step_u = 1 + (side - 1) * core
    step_v = side - (side - 1) * core

    def chip_of(uu, vv):
        return vv * step_v + uu * step_u

    def wrap(value):
        return lax.rem(value + 2 * side, side)

    def remote(src, dst, send, recv, target):
        pltpu.make_async_remote_copy(
            src_ref=src, dst_ref=dst, send_sem=send, recv_sem=recv,
            device_id={"wide": target}, device_id_type=pl.DeviceIdType.MESH,
        ).start()

    def await_bytes(ref, sem):
        pltpu.make_async_copy(ref, ref, sem).wait()

    own_x = pltpu.make_async_copy(xa_hbm, gathered.at[chip, core, 0], own_sem.at[0])
    own_z = pltpu.make_async_copy(za_hbm, gathered.at[chip, core, 1], own_sem.at[1])
    own_x.start()
    own_z.start()

    at_u = {o: wrap(u + o) for o in range(-(side // 2) + 1, side // 2 + 1)}
    at_v = {o: wrap(v + o) for o in range(-2, 3)}
    to_u = {o: chip_of(at_u[o], v) * 2 + core for o in at_u if o}
    to_v = {o: chip_of(u, at_v[o]) * 2 + core for o in at_v if o}
    barrier = pltpu.get_barrier_semaphore()
    partners = list(to_u.values()) + list(to_v.values()) + [sibling]
    for partner in partners:
        pl.semaphore_signal(
            barrier, inc=1, device_id={"wide": partner}, device_id_type=pl.DeviceIdType.MESH
        )
    a_copy = pltpu.make_async_copy(a_hbm, a_vmem, a_sem)
    send_copy = pltpu.make_async_copy(send_hbm, send_ref, order_sem.at[0])
    recv_copy = pltpu.make_async_copy(recv_hbm, recv_ref, order_sem.at[1])
    a_copy.start()
    send_copy.start()
    shift_copy = pltpu.make_async_copy(shift_hbm, shift_ref, order_sem.at[2])
    recv_copy.start()
    shift_copy.start()
    own_x.wait()
    own_z.wait()
    pl.semaphore_wait(barrier, len(partners))

    def send_block(block_chip, target, send, recv):
        block = gathered.at[block_chip, core]
        remote(block, block, send, recv, target)

    half = side // 2
    groups = u_groups(side)
    group_of = {o: g for g, members in enumerate(groups) for o in members}
    across = ((0, len(groups) - 1), tuple(range(1, len(groups) - 1)))
    signs = (1, -1)
    for o in sorted(to_u, key=lambda o: -abs(o)):
        send_block(chip, to_u[o], ag_send.at[0], ag_recv_u.at[group_of[o]])

    def blocks_of(g, row):
        return [chip_of(at_u[o], row) for o in groups[g]]

    def send_v(g, row, hop, way, jump):
        for block in blocks_of(g, row):
            send_block(
                block, to_v[signs[way] * jump], ag_send.at[1], ag_recv_v.at[way, hop - 1, g]
            )

    def share(g, row):
        for block in blocks_of(g, row):
            send_block(block, sibling, ag_send.at[2], ag_recv_s)

    def arrived(g, hop, way):
        await_bytes(gathered.at[0 : len(groups[g]), 0], ag_recv_v.at[way, hop - 1, g])

    for g in range(len(groups)):
        if g > 0:
            await_bytes(gathered.at[0 : len(groups[g]), 0], ag_recv_u.at[g])
        for jump in (2, 1):
            for way in range(2):
                send_v(g, v, jump, way, jump)
        share(g, v)
    for g in range(len(groups)):
        for way in range(2):
            arrived(g, 2, way)
            row = at_v[-2 * signs[way]]
            if g in across[way]:
                send_v(g, row, 4, way, 2)
            send_v(g, row, 3, way, 1)
            share(g, row)
        for way in range(2):
            arrived(g, 1, way)
            share(g, at_v[-signs[way]])
    for g in range(len(groups)):
        for way in range(2):
            arrived(g, 3, way)
            share(g, wrap(v - 3 * signs[way]))
            if g in across[way]:
                arrived(g, 4, way)
                share(g, wrap(v - 4 * signs[way]))
    a_copy.wait()
    send_copy.wait()
    recv_copy.wait()
    shift_copy.wait()
    await_bytes(gathered.at[:, 0], ag_recv_s)

    tile = rows // 4
    depth = a_vmem.shape[1]

    def product(t, _):
        at = pl.ds(pl.multiple_of(t * tile, tile), tile)
        lhs = a_vmem[at, :]
        cols = gathered.shape[-1]
        one = jnp.dot(lhs, gathered[:, :, 0].reshape(depth, cols), preferred_element_type=F32)
        two = jnp.dot(lhs, gathered[:, :, 1].reshape(depth, cols), preferred_element_type=F32)
        schur = one * two
        sa[at, :] = schur[:, :LANES]
        sr[at, :] = pltpu.roll(schur[:, :LANES], PANEL, 1)
        sb[at, :] = schur[:, LANES:]
        return 0

    lax.fori_loop(0, 4, product, 0)

    low = lane_iota((1, LANES)) < PANEL

    def pack_lead(e, _):
        firsts, seconds = [], []
        for k in range(pair):
            firsts.append(sa[pl.ds(send_ref[0, e * per + k], 1), :])
            seconds.append(sr[pl.ds(send_ref[0, e * per + pair + k], 1), :])
        for k in range(pair):
            lead_out[e, pl.ds(k, 1), :] = jnp.where(low, firsts[k], seconds[k])
        return 0

    def send_to(e, source, target_ref, send, recv):
        @pl.when(e != me)
        def _():
            remote(source.at[e], target_ref.at[me], send, recv, e)

    def mixed(i):
        return lax.rem(me + i * SPREAD, n)

    def lead_first(i, _):
        e = start_lead + i
        e = jnp.where(e >= n_lead, e - n_lead, e)

        @pl.when(e != 0)
        def _():
            send_to(e, lead_out, lead_in, lead_send, lead_recv)

        return 0

    def lead_other(i, _):
        e = mixed(i)

        @pl.when(e >= n_lead)
        def _():
            send_to(e, lead_out, lead_in, lead_send, lead_recv)

        return 0

    start_lead = lax.rem(me, n_lead)
    assert math.gcd(SPREAD, n) == 1
    lax.fori_loop(0, n_lead, pack_lead, 0)
    send_to(0, lead_out, lead_in, lead_send, lead_recv)
    lax.fori_loop(n_lead, n, pack_lead, 0)
    lax.fori_loop(0, n_lead, lead_first, 0)
    lax.fori_loop(1, n, lead_other, 0)
    lead_in[me] = lead_out[me]

    magic = -(-65536 // per)
    assert all((j * magic) >> 16 == j // per for j in range(rows))

    def find_slots(i, _):
        for k in range(8):
            slot = recv_ref[0, i * 8 + k]
            source = lax.shift_right_logical(slot * magic, 16)
            slots[0, i * 8 + k] = slot + (16 - per) * source
        return 0


    flat_a = both_a.reshape(n * 16, LANES)
    flat_b = rest_g.reshape(n * 16, LANES)

    def take(source, start):
        return jnp.concatenate(
            [source[pl.ds(slots[0, start + k], 1), :] for k in range(8)], axis=0
        )

    def take_leads():
        await_bytes(lead_in.at[0 : n - 1], lead_recv)

        def spread_lead(i, _):
            at = pl.ds(i * 8, 8)
            values = lead_in[at]
            both_a[at, 0:pair] = values
            both_a[at, pair : 2 * pair] = pltpu.roll(values, PANEL, 2)
            return 0

        lax.fori_loop(0, n // 8, spread_lead, 0)

    hp = PANEL // 2
    group = 2 * side
    levels = -(-n_lead // group)

    def publish():
        lax.fori_loop(0, PANEL // 8, find_slots, 0)
        take_leads()

        def first(i, _):
            first_rows[pl.ds(pl.multiple_of(i * 8, 8), 8), :] = take(flat_a, i * 8)
            return 0

        lax.fori_loop(0, PANEL // 8, first, 0)
        packed = jnp.where(
            low, first_rows[0:hp, :], pltpu.roll(first_rows[hp:PANEL, :], PANEL, 1)
        )
        leading_src[...] = packed
        leading[me] = packed
        for i in sorted(range(1, side), key=lambda i: -min(i, side - i)):
            target = (wrap(y + i) * side + x) * 2 + core
            remote(leading_src, leading.at[me], tree_send1, tree_recv1.at[y], target)

    def relay(m, e):
        @pl.when(y != m)
        def _():
            await_bytes(leading.at[0], tree_recv1.at[m])

        for i in sorted(range(1, side), key=lambda i: -min(i, side - i)):
            target = (y * side + wrap(x + i)) * 2 + core
            remote(leading.at[e], leading.at[e], tree_send2.at[m], tree_recv2.at[e], target)
        remote(leading.at[e], leading.at[e], tree_send3.at[e], tree_recv3.at[e], sibling)

    @pl.when(me == 0)
    def _():
        publish()
        relay(0, 0)

    def pack_rest(e, _):
        parts = []
        for k in range(pair):
            one = send_ref[0, e * per + k]
            two = send_ref[0, e * per + pair + k]
            parts.append((
                sb[pl.ds(one, 1), :], sb[pl.ds(two, 1), :],
                sr[pl.ds(one, 1), :], sa[pl.ds(two, 1), :],
            ))
        for k in range(pair):
            one, two, left, right = parts[k]
            rest_f[e, pl.ds(k, 1), :] = one
            rest_f[e, pl.ds(pair + k, 1), :] = two
            rest_f[e, pl.ds(2 * pair + k, 1), :] = jnp.where(low, left, right)
        return 0

    rest_f[:, 3 * pair :, :] = jnp.zeros((n, 16 - 3 * pair, LANES), F32)
    lax.fori_loop(0, n, pack_rest, 0)

    def quantize(i, _):
        at = pl.ds(i * 8, 8)
        values = rest_f[at]
        largest = jnp.max(jnp.abs(values), axis=1, keepdims=True)
        power = jnp.floor(jnp.log2(jnp.maximum(largest, 1e-30))) + 1.0
        scale = Q_MAX / jnp.exp2(power)
        coded = jnp.clip(jnp.round(values * scale), -Q_MAX, Q_MAX)
        spot = lax.broadcasted_iota(jnp.int32, values.shape, 1)
        coded = jnp.where(spot == 3 * pair, power, coded)
        rest_out[at] = coded.astype(jnp.int32).astype(jnp.int16)
        return 0

    lax.fori_loop(0, n // 8, quantize, 0)

    chunks = 8
    span = n // chunks
    my_chunk = lax.div(me, span)

    def send_rest(i, _):
        send_to(mixed(i), rest_out, rest_in, rest_send, rest_recv.at[my_chunk])
        return 0

    on_path = (x == 0) & (core == 0)
    relays_first = (me < n_lead) | on_path

    @pl.when(jnp.logical_not(relays_first))
    def _():
        lax.fori_loop(1, n, send_rest, 0)

    @pl.when(on_path & (me > 0))
    def _():
        relay(0, 0)

    @pl.when((me < n_lead) & (me > 0))
    def _():
        publish()

    @pl.when(relays_first)
    def _():
        lax.fori_loop(1, n, send_rest, 0)

    rest_in[me] = rest_out[me]
    lax.fori_loop(0, rows // 8, find_slots, 0)

    @pl.when(me >= n_lead)
    def _():
        take_leads()

    def pass_on(e):
        await_bytes(leading.at[0], tree_recv2.at[e])
        remote(leading.at[e], leading.at[e], tree_send3.at[e], tree_recv3.at[e], sibling)

    @pl.when((x != 0) & (core == 0))
    def _():
        pass_on(0)

    @pl.when(core == 1)
    def _():
        await_bytes(leading.at[0], tree_recv3.at[0])

    eliminate_block(leading[0], shift_ref, work, lower_ref, pivots_ref)

    for m in range(levels):
        e = m * group + 2 * x + core

        @pl.when((e < n_lead) & (e > 0))
        def _(m=m, e=e):
            relay(m, e)

    def spread_rest(i, _):
        at = pl.ds(i * 8, 8)
        coded = rest_in[at].astype(jnp.int32).astype(F32)
        power = coded[:, 3 * pair : 3 * pair + 1]
        values = coded * (jnp.exp2(power) / Q_MAX)
        rest_g[at] = values
        mid = values[:, 2 * pair : 3 * pair]
        kept = lane_iota(mid.shape) < PANEL
        both_a[at, 0:pair] = jnp.where(kept, both_a[at, 0:pair], pltpu.roll(mid, PANEL, 2))
        both_a[at, pair : 2 * pair] = jnp.where(kept, both_a[at, pair : 2 * pair], mid)
        return 0

    for chunk in range(chunks):
        at = chunk * span

        @pl.when(my_chunk == chunk)
        def _(chunk=chunk, at=at):
            await_bytes(rest_in.at[at : at + span - 1], rest_recv.at[chunk])

        @pl.when(my_chunk != chunk)
        def _(chunk=chunk, at=at):
            await_bytes(rest_in.at[at : at + span], rest_recv.at[chunk])

        lax.fori_loop(at // 8, (at + span) // 8, spread_rest, 0)

    for m in range(levels):
        for i in range(1, side):
            e = m * group + 2 * wrap(x + i) + core

            @pl.when((e < n_lead) & (e > 0))
            def _(e=e):
                pass_on(e)

    def place(i, _):
        at = pl.ds(pl.multiple_of(i * 8, 8), 8)
        stored_a[at, :] = take(flat_a, i * 8)
        stored_b[at, :] = take(flat_b, i * 8)
        return 0

    lax.fori_loop(0, rows // 8, place, 0)

    def from_sibling(e, _):
        @pl.when(lax.rem(e, 2) != core)
        def _():
            await_bytes(leading.at[0], tree_recv3.at[e])

        return 0

    lax.fori_loop(1, n_lead, from_sibling, 0)

    await_bytes(gathered.at[0 : side - 1, 0], ag_send.at[0])
    await_bytes(gathered.at[0 : side * (side - 1), 0], ag_send.at[1])
    await_bytes(gathered.at[:, 0], ag_send.at[2])
    await_bytes(lead_out.at[0 : n - 1], lead_send)
    await_bytes(rest_out.at[0 : n - 1], rest_send)

    @pl.when(me < n_lead)
    def _():
        await_bytes(leading.at[0 : side - 1], tree_send1)

    for m in range(levels):
        e = m * group + 2 * x + core

        @pl.when(e < n_lead)
        def _(m=m):
            await_bytes(leading.at[0 : side - 1], tree_send2.at[m])

    def to_sibling(e, _):
        @pl.when(lax.rem(e, 2) == core)
        def _():
            await_bytes(leading.at[0], tree_send3.at[e])

        return 0

    lax.fori_loop(0, n_lead, to_sibling, 0)


def eliminate_block(head, shift_ref, work, lower_ref, pivots_ref):
    turned = pltpu.roll(head, PANEL, 1)
    block = jnp.concatenate([head, turned], axis=0)
    r = lax.broadcasted_iota(jnp.int32, block.shape, 0)
    c = lane_iota(block.shape)
    inside = c < PANEL
    strict = jnp.where((r > c) & inside, block, 0.0)
    pad = jnp.concatenate([strict, jnp.zeros_like(strict)], axis=0)
    mirrored = jnp.where((r >= c) & inside, block, 0.0) + pad.T[:PANEL, :]
    magnitude = jnp.sum(jnp.abs(mirrored), axis=0, keepdims=True)
    shift = shift_ref[...].reshape(1, PANEL)
    diagonal = magnitude + jnp.concatenate([shift, shift], axis=1)
    start = jnp.where(r == c, diagonal, mirrored)
    work[...] = jnp.where(inside, start, jnp.where(r == c - PANEL, 1.0, 0.0))
    lower_ref[...] = jnp.zeros_like(block)

    lane = lane_iota((1, LANES))

    def pick(values, mask):
        return jnp.sum(jnp.where(mask, values, 0.0), axis=1, keepdims=True)

    def eliminate(i, pivots):
        j = 2 * i
        matrix = work[...]
        row0 = work[pl.ds(j, 1), :]
        row1 = work[pl.ds(j + 1, 1), :]
        column0 = pick(matrix, c == j)
        column1 = pick(matrix, c == j + 1)
        pivot0 = pick(row0, lane == j)
        beside = pick(row0, lane == j + 1)
        under = pick(row1, lane == j)
        corner = pick(row1, lane == j + 1)
        inverse0 = 1.0 / pivot0
        ratio = under * inverse0
        below0 = jnp.where(r > j, column0 * inverse0, 0.0)
        row1 = row1 - ratio * row0
        pivot1 = corner - ratio * beside
        below1 = jnp.where(r > j + 1, (column1 - below0 * beside) * (1.0 / pivot1), 0.0)
        work[...] = matrix - below0 * row0 - below1 * row1
        new0 = below0 + jnp.where(r == j, 1.0, 0.0)
        new1 = below1 + jnp.where(r == j + 1, 1.0, 0.0)
        lower_ref[...] += jnp.where(c == j, new0, jnp.where(c == j + 1, new1, 0.0))
        return jnp.where(lane == j, pivot0, jnp.where(lane == j + 1, pivot1, pivots))

    pivots_ref[...] = lax.fori_loop(0, PANEL // 2, eliminate, jnp.ones((1, LANES), F32))


def exchange(n, n_lead, a_rows, xa, za, send_order, recv_order, shift):
    rows, depth = a_rows.shape
    cols = xa.shape[1]
    share = xa.shape[0]
    per = rows // n
    pair = per // 2
    side = math.isqrt(n // 2)
    hp = PANEL // 2
    dma = pltpu.SemaphoreType.DMA
    hbm = pl.BlockSpec(memory_space=pltpu.HBM)
    vmem = pl.BlockSpec(memory_space=pltpu.VMEM)
    levels = -(-n_lead // (2 * side))
    n_groups = len(u_groups(side))
    return pl.pallas_call(
        functools.partial(exchange_kernel, n, n_lead),
        out_shape=(
            jax.ShapeDtypeStruct((rows, LANES), F32),
            jax.ShapeDtypeStruct((rows, LANES), F32),
            jax.ShapeDtypeStruct((n_lead, hp, LANES), F32),
            jax.ShapeDtypeStruct((PANEL, LANES), F32),
            jax.ShapeDtypeStruct((PANEL, LANES), F32),
            jax.ShapeDtypeStruct((1, LANES), F32),
        ),
        in_specs=[hbm] * 6,
        out_specs=(vmem,) * 6,
        scratch_shapes=[
            pltpu.VMEM((rows, depth), BF16),
            pltpu.VMEM((n // 2, 2, 2, share, cols), BF16),
            pltpu.VMEM((rows, LANES), F32),
            pltpu.VMEM((rows, LANES), F32),
            pltpu.VMEM((rows, LANES), F32),
            pltpu.VMEM((n, pair, LANES), F32),
            pltpu.VMEM((n, 16, LANES), F32),
            pltpu.VMEM((n, 16, LANES), jnp.int16),
            pltpu.VMEM((n, pair, LANES), F32),
            pltpu.VMEM((n, 16, LANES), jnp.int16),
            pltpu.VMEM((n, 16, LANES), F32),
            pltpu.VMEM((n, 16, LANES), F32),
            pltpu.VMEM((PANEL, LANES), F32),
            pltpu.VMEM((hp, LANES), F32),
            pltpu.VMEM((PANEL,), F32),
            pltpu.SMEM((1, rows), jnp.int32),
            pltpu.SMEM((1, rows), jnp.int32),
            pltpu.SMEM((1, rows), jnp.int32),
            dma, dma((2,)), dma((3,)), dma((3,)), dma((n_groups,)), dma((2, 4, n_groups)), dma,
            dma, dma, dma, dma((8,)),
            dma, dma((levels,)), dma((n_lead,)), dma((side,)), dma((n_lead,)), dma((n_lead,)),
        ],
        compiler_params=pltpu.CompilerParams(
            collective_id=0, has_side_effects=True, vmem_limit_bytes=48 * 1024 * 1024
        ),
    )(*(pltpu.with_memory_space_constraint(o, pltpu.HBM) for o in (
        a_rows, xa, za, send_order, recv_order, shift
    )))


def two_parts(values):
    high = values.astype(BF16)
    return high, (values - high.astype(F32)).astype(BF16)


def left_stack(twice):
    high, mid = two_parts(twice)
    return jnp.concatenate([high, mid], axis=1)


def right_stack(twice):
    high, mid = two_parts(twice)
    once = jnp.where(lane_iota(twice.shape) < PANEL, high.astype(F32), mid.astype(F32))
    once = once.astype(BF16)
    return jnp.concatenate([once, once], axis=1)


def dot_nt(a, b):
    return lax.dot_general(a, b, (((1,), (1,)), ((), ())), preferred_element_type=F32)


def finish_kernel(
    a_ref, b_ref, leading, work, lower_ref, pivot_ref, resident_ref,
    factored_ref, updated_ref, pivots_ref,
    inverse_ref, tail_ref,
):
    step = pl.program_id(0)
    me = lax.axis_index("wide")
    tile = a_ref.shape[0]

    @pl.when(step == 0)
    def _():
        final = work[...]
        inside = lane_iota(final.shape) < PANEL
        pivots_ref[...] = pivot_ref[...][0, :PANEL]
        inverse = jnp.where(inside, pltpu.roll(final, PANEL, 1), final)
        inverse_ref[0:PANEL, :] = right_stack(inverse)
        inverse_ref[PANEL:, :] = jnp.zeros_like(inverse_ref[PANEL:, :])
        blocks = leading[...]
        keep = lane_iota(blocks.shape) < PANEL
        other = pltpu.roll(blocks, PANEL, 2)
        top = jnp.where(keep, blocks, other)
        bottom = jnp.where(keep, other, blocks)
        full = jnp.concatenate([top, bottom], axis=1)
        full = full.reshape(full.shape[0] * PANEL, LANES)
        tail = dot_nt(left_stack(full), inverse_ref[...])
        tail = tail + pltpu.roll(tail, PANEL, 1)
        place = lax.broadcasted_iota(jnp.int32, tail.shape, 0)
        tail_ref[...] = right_stack(jnp.where(place < PANEL, 0.0, tail))

    a = a_ref[...]
    lanes = lane_iota(a.shape)
    local = lax.broadcasted_iota(jnp.int32, a.shape, 0) + step * tile
    low = lanes < PANEL
    lead = jnp.where(low, a, pltpu.roll(a, PANEL, 1))
    scaled = dot_nt(left_stack(lead), inverse_ref[...])
    panel = scaled / pivot_ref[...]
    is_top = (local < PANEL) & (me == 0)
    fill = tile // PANEL
    lower = jnp.concatenate([lower_ref[...]] * fill, axis=0)
    panel = jnp.where(is_top, lower, panel)
    update = dot_nt(left_stack(panel + pltpu.roll(panel, PANEL, 1)), tail_ref[...])
    cols = b_ref.shape[1] + a.shape[1]

    def kept(values):
        rows_at = lax.broadcasted_iota(jnp.int32, values.shape, 0) + step * tile
        return jnp.where((rows_at < PANEL) & (me == 0), 0.0, values)

    factored_ref[:, :LANES] = jnp.where(low, panel, a - kept(update[:, :LANES]))
    factored_ref[:, LANES:] = b_ref[...] - kept(update[:, LANES:cols])
    updated_ref[...] = (resident_ref[...].astype(F32) - kept(update[:, cols:])).astype(BF16)


def finish(stored_a, stored_b, leading, work, lower, pivots, resident):
    rows = stored_a.shape[0]
    tile = 256
    width = resident.shape[1]
    cols = stored_a.shape[1] + stored_b.shape[1]
    n_lead = leading.shape[0]
    row_spec = lambda w: pl.BlockSpec((tile, w), lambda i: (i, 0))
    whole = lambda shape: pl.BlockSpec(shape, lambda i: (0,) * len(shape))
    return pl.pallas_call(
        finish_kernel,
        grid=(rows // tile,),
        out_shape=(
            jax.ShapeDtypeStruct((rows, cols), F32),
            jax.ShapeDtypeStruct((rows, width), BF16),
            jax.ShapeDtypeStruct((PANEL,), F32),
        ),
        in_specs=[
            row_spec(LANES), row_spec(LANES), whole(leading.shape), whole(work.shape),
            whole(lower.shape), whole(pivots.shape), row_spec(width),
        ],
        out_specs=(row_spec(cols), row_spec(width), whole((PANEL,))),
        scratch_shapes=[
            pltpu.VMEM((LANES, 2 * LANES), BF16),
            pltpu.VMEM((n_lead * PANEL, 2 * LANES), BF16),
        ],
        compiler_params=pltpu.CompilerParams(vmem_limit_bytes=32 * 1024 * 1024),
    )(stored_a, stored_b, leading, work, lower, pivots, resident)


def on_device(n, a_rows, xa_panel, za_panel, send_order, recv_order, shift, resident):
    needed = xa_panel.shape[1] + resident.shape[1]
    n_lead = -(-needed // PANEL)
    stored_a, stored_b, leading, work, lower, pivots = exchange(
        n, n_lead, a_rows, xa_panel, za_panel, send_order, recv_order, shift
    )
    return finish(stored_a, stored_b, leading, work, lower, pivots, resident)


def solution(mesh):
    spread = P(("parts", "wide"), None)
    return jax.shard_map(
        functools.partial(on_device, mesh.shape["wide"]),
        mesh=mesh,
        in_specs=(spread, spread, spread, spread, spread, P("parts"), spread),
        out_specs=(spread, spread, P("parts")),
        check_vma=False,
    )
```
